32 devices in a mesh: seq: 4 (over x, core), vocab: 8 (over z, y).
Axes of the slice: x: 2, y: 2, z: 4, core: 2. Of those that a mesh axis runs over, the one named last changes fastest.
Arguments:
- hidden: bfloat16 [512, 4608], P('seq', 'vocab'), may hold values from -6 to 6
- norm_gain: float32 [4608], replicated, may hold values from -1.5 to 1.5
- unembed: bfloat16 [256000, 4608], P(('seq', 'vocab')), may hold values from -0.375 to 0.375
- targets: int32 [512], P('seq'), may hold values from 0 to 255999
Outputs:
- log_prob: float32 [512], P('seq')
- entropy: float32 [512], P('seq')
The draws below stay inside these ranges and needn't reach their ends.
All inputs are finite; a program needn't handle non-finite values.
Results may differ from the reference program's by a relative error of at most 0.0012.
Values may be sent and summed in bfloat16 or wider, within the bound.
No kernel may reach another device: no remote copies, remote signals or barrier semaphores. Data moves between devices by JAX's collectives and lax.ppermute only.
A program may use at most 128 MiB of HBM per device.

```python
import jax
import jax.numpy as jnp
from jax import lax

D = 4608
VOCAB = 256000
TOKENS = 512


def touch_ends(values, stream_key, low, top_value):
    longest = values.shape.index(max(values.shape))
    spots = []
    for shift in (0, 1):
        where = [jax.random.randint(jax.random.fold_in(stream_key, axis), (), 0, length) for axis, length in enumerate(values.shape)]
        where[longest] = (where[longest] + shift) % values.shape[longest]
        spots.append(tuple(where))
    return values.at[spots[0]].set(low).at[spots[1]].set(top_value)


def block_levels(key, extent, split, least, largest):
    level = 1.0
    for dim, blocks in split:
        heights = jax.random.uniform(jax.random.fold_in(jax.random.fold_in(key, 6), dim), (blocks,), jnp.float32, least / len(split), largest / len(split))
        level = level * jnp.repeat(jnp.exp(heights), extent[dim] // blocks).reshape((-1,) + (1,) * (len(extent) - 1 - dim))
    return level


def centred(rng, dims, spread, reach, pieces=(), kind=jnp.bfloat16):
    result = spread * jax.random.normal(rng, dims, jnp.float32)
    if pieces:
        result = result * block_levels(rng, dims, pieces, -0.22, 0.18)
    return jnp.clip(result, -reach, reach).astype(kind)


def setup_inputs(seed: int = 0) -> dict:
    splits = jax.random.split(jax.random.key(seed), 5)
    return {
        "hidden": centred(splits[0], (TOKENS, D), 1.0, 6.0, ((0, 4), (1, 8))),
        "norm_gain": centred(splits[1], (D,), 0.3, 1.5, (), jnp.float32),
        "unembed": centred(splits[2], (VOCAB, D), (D // 16) ** -0.5, 0.375, ((0, 32),)),
        "targets": touch_ends(jax.random.randint(splits[3], (TOKENS,), 0, VOCAB), jax.random.fold_in(splits[3], 1), 0, VOCAB - 1).astype(jnp.int32),
    }


softcap = 30.0
epsilon = 1e-06

def normalize(hidden, norm_gain):
    values = hidden.astype(jnp.float32)
    scale = lax.rsqrt(lax.optimization_barrier(jnp.mean(values * values, axis=1, keepdims=True)) + epsilon)
    return (values * scale * (1.0 + norm_gain.astype(jnp.float32))).astype(jnp.bfloat16)

def reference(hidden, norm_gain, unembed, targets):
    normed = normalize(hidden, norm_gain)
    blocks = unembed.reshape(32, VOCAB // 32, D)

    def block_sums(block):
        logits = lax.dot_general(normed, block, (((1,), (1,)), ((), ())), preferred_element_type=jnp.float32)
        capped = softcap * jnp.tanh(logits / softcap)
        weights = jnp.exp(capped - softcap)
        return (lax.optimization_barrier(jnp.sum(weights, axis=1)), lax.optimization_barrier(jnp.sum(weights * capped, axis=1)))
    sums, moments = lax.map(block_sums, blocks)
    total = lax.optimization_barrier(jnp.sum(sums, axis=0))
    moment = lax.optimization_barrier(jnp.sum(moments, axis=0))
    picked = unembed[targets.astype(jnp.int32)].astype(jnp.float32)
    target_logit = lax.optimization_barrier(jnp.sum(normed.astype(jnp.float32) * picked, axis=1))
    chosen = softcap * jnp.tanh(target_logit / softcap)
    log_norm = softcap + jnp.log(total)
    return (chosen - log_norm, log_norm - moment / total)
```

```python
import functools

import jax
import jax.numpy as jnp
from jax import lax
from jax.experimental import pallas as pl
from jax.experimental.pallas import tpu as pltpu
from jax.sharding import PartitionSpec as P

softcap = 30.0
epsilon = 1e-06


def fill(info, pieces, spots, weights, width, own_tokens):
    for piece, placed in zip(pieces, spots):
        for j, (dv, ds) in enumerate(placed):
            row = pl.multiple_of((info[0] ^ dv) * width, width)
            weights[pl.ds(row, width), ds * own_tokens : (ds + 1) * own_tokens] = piece[j]


def body(info, u, scale, wanted, *rest, spots, width, own_tokens, chunk):
    pieces, (out, weights) = rest[:-2], rest[-2:]
    step = pl.program_id(0)

    @pl.when(step == 0)
    def _():
        fill(info, pieces, spots, weights, width, own_tokens)
        out[...] = jnp.zeros_like(out)

    rows = u.shape[0]
    tokens = weights.shape[1]
    by_scale = scale[...] * (1.0 / softcap)
    sums = [jnp.zeros((8, tokens), jnp.float32) for _ in range(3)]
    for start in range(0, rows, chunk):
        logits = jnp.dot(u[start : start + chunk, :], weights[...], preferred_element_type=jnp.float32)
        capped = softcap * jnp.tanh(logits * by_scale)
        each = jnp.exp(capped - softcap)
        row = lax.broadcasted_iota(jnp.int32, logits.shape, 0)
        hit = row == wanted[...] - (info[1] + step * rows + start)
        for k, value in enumerate((each, each * capped, jnp.where(hit, capped, 0.0))):
            sums[k] = sums[k] + jnp.sum(value.reshape(chunk // 8, 8, tokens), axis=0)
    for k in range(3):
        out[k : k + 1, :] += jnp.sum(sums[k], axis=0, keepdims=True)


def on_device(hidden, norm_gain, unembed, targets, sizes):
    n_seq, n_vocab = sizes
    vocab_rows, features = unembed.shape
    own_tokens, width = hidden.shape
    tokens = own_tokens * n_seq
    top = n_vocab // 2
    seq = lax.axis_index("seq")
    vocab = lax.axis_index("vocab")

    def swap(value, axis, bit):
        size = n_seq if axis == "seq" else n_vocab
        return lax.ppermute(value, axis, [(i, i ^ bit) for i in range(size)])

    gain = lax.dynamic_slice_in_dim(norm_gain, vocab * width, width)
    values = hidden.T.astype(jnp.float32)
    block = (values * (1.0 + gain)[:, None]).astype(jnp.bfloat16)[None]
    squares = jnp.sum(values * values, axis=0)

    def doubled(piece, spot, axis, bit):
        step = (bit, 0) if axis == "vocab" else (0, bit)
        return swap(piece, axis, bit), [(v ^ step[0], s ^ step[1]) for v, s in spot]

    inner = [("vocab", 1 << b) for b in range(1, top.bit_length() - 1)]
    inner += [("seq", 1 << b) for b in range(1, (n_seq // 2).bit_length() - 1)]
    line, across = ("vocab", 1), ("seq", n_seq // 2)

    def assemble(piece, far):
        spot = [(0, 0)]
        for axis, bit in inner:
            other, moved = doubled(piece, spot, axis, bit)
            piece = jnp.concatenate([piece, other])
            spot = spot + moved
        one = (piece, spot)
        two = doubled(*one, *line)
        three = doubled(*one, *across)
        four = doubled(*three, *line) if far else doubled(*two, *across)
        found = [one, two, three, four]
        found += [doubled(*p, "seq", 1) for p in found]
        return [p for p, _ in found], [s for _, s in found]

    far_block = swap(block, "vocab", top)
    near, spots = assemble(block, False)
    away, away_spots = assemble(far_block, True)

    bit = 1
    while bit < n_vocab:
        squares = squares + swap(squares, "vocab", bit)
        bit *= 2
    small = jnp.stack([squares, targets.astype(jnp.float32)])[None]
    bit = 1
    while bit < n_seq:
        small = jnp.concatenate([small, swap(small, "seq", bit)])
        bit *= 2
    scale = lax.rsqrt(small[:, 0] / features + epsilon).reshape(1, tokens)
    wanted = small[:, 1].astype(jnp.int32).reshape(1, tokens)

    away_spots = [[(v ^ top, s) for v, s in spot] for spot in away_spots]
    pieces = near + away
    first = (seq * n_vocab + vocab) * vocab_rows
    rows = max(r for r in range(16, 801, 16) if vocab_rows % r == 0)
    chunk = max(c for c in range(16, 400 + 1, 16) if rows % c == 0)

    def whole(shape):
        return pl.BlockSpec(shape, lambda i, info: (0,) * len(shape))

    stats = pl.pallas_call(
        functools.partial(body, spots=spots + away_spots, width=width, own_tokens=own_tokens, chunk=chunk),
        out_shape=jax.ShapeDtypeStruct((3, tokens), jnp.float32),
        grid_spec=pltpu.PrefetchScalarGridSpec(
            num_scalar_prefetch=1,
            grid=(vocab_rows // rows,),
            in_specs=[pl.BlockSpec((rows, features), lambda i, info: (i, 0)), whole((1, tokens)), whole((1, tokens))]
            + [whole(p.shape) for p in pieces],
            out_specs=whole((3, tokens)),
            scratch_shapes=[pltpu.VMEM((features, tokens), jnp.bfloat16)],
        ),
        compiler_params=pltpu.CompilerParams(dimension_semantics=("arbitrary",), vmem_limit_bytes=52 * 2**20),
        name="vocab_stats",
    )(jnp.stack([vocab, first]), unembed, scale, wanted, *pieces)

    bit = n_seq // 2
    while bit:
        stats = stats[:, : bit * own_tokens] + swap(stats[:, bit * own_tokens :], "seq", bit)
        bit //= 2
    bit = 1
    while bit < n_vocab:
        stats = stats + swap(stats, "vocab", bit)
        bit *= 2
    total, moment, chosen = stats
    log_norm = softcap + jnp.log(total)
    return (chosen - log_norm, log_norm - moment / total)


def solution(mesh):
    sizes = (mesh.shape["seq"], mesh.shape["vocab"])
    return jax.shard_map(
        functools.partial(on_device, sizes=sizes),
        mesh=mesh,
        in_specs=(P("seq", "vocab"), P(), P(("seq", "vocab"), None), P("seq")),
        out_specs=(P("seq"), P("seq")),
        check_vma=False,
    )
```
